32 devices in a mesh: dp: 2 (over z, core), tp: 16 (over x, y).
Axes of the slice: x: 4, y: 4, z: 1, core: 2. Of those that a mesh axis runs over, the one named last changes fastest.
The devices are a block of a 4x4x8 slice.
Arguments:
- x: bfloat16 [4096, 8192], P('dp'), parts along dimension 0
- w_gate: bfloat16 [8192, 28672], P(None, 'tp')
- w_up: bfloat16 [8192, 28672], P(None, 'tp')
- w_down: bfloat16 [28672, 8192], P('tp')
Outputs:
- output: bfloat16 [4096, 8192], P('dp'), parts along dimension 0
There are 2 independent parts. The reference program is written for one: setup_inputs(seed, part) draws one part's arguments, and reference() takes and returns one part's arrays. A program takes and returns all parts, laid end to end along the dimension named above; an argument that names none is the same for every part.
All inputs are finite; a program needn't handle non-finite values.
Results may differ from the reference program's by a relative error of at most 0.016.
Values are sent between devices in bfloat16 or wider.
A program may use at most 768 MiB of HBM per device.

```python
import jax
import jax.numpy as jnp

ROWS = 2048
D = 8192
FF = 28672


def setup_inputs(seed: int = 0, part: int = 0) -> dict:
    kx, kg, ku, kd = jax.random.split(jax.random.key(seed), 4)
    drawn = {
        "x": jax.random.normal(jax.random.fold_in(kx, part), (ROWS, D), jnp.float32),
        "w_gate": jax.random.normal(kg, (D, FF), jnp.float32) * D**-0.5,
        "w_up": jax.random.normal(ku, (D, FF), jnp.float32) * D**-0.5,
        "w_down": jax.random.normal(kd, (FF, D), jnp.float32) * FF**-0.5,
    }
    return {k: v.astype(jnp.bfloat16) for k, v in drawn.items()}


def reference(x, w_gate, w_up, w_down):
    gate = jnp.dot(x, w_gate, preferred_element_type=jnp.float32)
    up = jnp.dot(x, w_up, preferred_element_type=jnp.float32)
    hidden = (jax.nn.silu(gate) * up).astype(jnp.bfloat16)
    return jnp.dot(hidden, w_down, preferred_element_type=jnp.float32).astype(jnp.bfloat16)
```

```python
import functools
import math

import jax
import jax.numpy as jnp
from jax import lax
from jax.experimental import pallas as pl
from jax.experimental.pallas import tpu as pltpu
from jax.sharding import PartitionSpec as P

CHUNK = 256
TILE = 256
WIDTH = 512
LAG = 3
DEPTH = 8
SENDS = 4
STEPS = 8


def kernel(
    side, x_hbm, wg_hbm, wu_hbm, wd_hbm, y_hbm,
    xbuf, wgu, both, wd, hid, term, part, s1, r1, s2, r2, t1, q1, t2, q2, fin,
    send_sem, recv_sem, x_sem, wgu_sem, wd_sem, own_sem,
):
    rows, d_model = x_hbm.shape
    units = wg_hbm.shape[1]
    chunks = rows // CHUNK
    half = d_model // 2
    per_chunk = half // WIDTH
    tiles = units // TILE
    items = chunks * per_chunk
    big, small = CHUNK // side, CHUNK // side // side
    cut = WIDTH // 2
    me = lax.axis_index("tp")
    pos = (me // side, lax.rem(me, side))

    def near(axis, step):
        at = lax.rem(pos[axis] + step + side, side)
        return at * side + pos[1] if axis == 0 else pos[0] * side + at

    def place(axis, step):
        return lax.rem(pos[axis] + step + side, side)

    barrier = pltpu.get_barrier_semaphore()
    for axis in (0, 1):
        for step in (1, -1):
            pl.semaphore_signal(
                barrier, inc=1, device_id={"tp": near(axis, step)},
                device_id_type=pl.DeviceIdType.MESH,
            )
    pl.semaphore_wait(barrier, 4)

    def copy(k, p, d, item):
        slot, out = lax.rem(item, DEPTH), lax.rem(item, SENDS)
        first, second = p, 1 - p
        axis = (first, first, second, second, second, second, first, first)[k]
        if k == 0:
            src, dst = s1.at[out, p, d], r1.at[slot, p, d]
        elif k == 1:
            src, dst = s2.at[out, p, d], r2.at[slot, p, d]
        elif k == 2:
            src, dst = t1.at[out, p, d], q1.at[slot, p, d]
        elif k == 3:
            src, dst = t2.at[out, p, d], q2.at[slot, p, d]
        else:
            row = lax.div(item, per_chunk) * CHUNK
            col = p * half + lax.rem(item, per_chunk) * WIDTH
            back = -1 if d == 0 else 1
            if k == 4:
                row += pos[first] * big + pos[second] * small
                height, wide = small, WIDTH
            elif k == 5:
                row += pos[first] * big + place(second, back) * small
                height, wide = small, cut
            elif k == 6:
                row += pos[first] * big
                height, wide = big, WIDTH
            else:
                row += place(first, back) * big
                height, wide = big, cut
            if k in (5, 7):
                col += d * cut
            dst = y_hbm.at[
                pl.ds(pl.multiple_of(row, small), height), pl.ds(pl.multiple_of(col, 128), wide)
            ]
            src = fin.at[out, p] if k == 4 else dst
        return pltpu.make_async_remote_copy(
            src_ref=src,
            dst_ref=dst,
            send_sem=send_sem.at[k, p, d, out],
            recv_sem=recv_sem.at[k, p, d, out],
            device_id={"tp": near(axis, 1 if d == 0 else -1)},
            device_id_type=pl.DeviceIdType.MESH,
        )

    def own_copy(p, item):
        out = lax.rem(item, SENDS)
        row = lax.div(item, per_chunk) * CHUNK + pos[p] * big + pos[1 - p] * small
        col = p * half + lax.rem(item, per_chunk) * WIDTH
        return pltpu.make_async_copy(
            fin.at[out, p],
            y_hbm.at[pl.ds(pl.multiple_of(row, small), small), pl.ds(pl.multiple_of(col, 128), WIDTH)],
            own_sem.at[out, p],
        )

    def start_all(k, item):
        for p in (0, 1):
            for d in (0, 1):
                copy(k, p, d, item).start()

    def wait_all(k, item):
        for p in (0, 1):
            for d in (0, 1):
                one = copy(k, p, d, item)
                one.wait_send()
                one.wait_recv()

    low, high = pl.ds(0, cut), pl.ds(cut, cut)

    def block(level, item, p, step, cols):
        slot = lax.rem(item, SENDS)
        if level == 0:
            return term[slot, p, pl.ds(pl.multiple_of(place(p, step) * big, big), big), cols]
        return part[slot, p, pl.ds(pl.multiple_of(place(1 - p, step) * small, small), small), cols]

    def send_first(level, item):
        out = lax.rem(item, SENDS)
        stage = (s1, t1)[level]
        for p in (0, 1):
            stage[out, p, 0, :, low] = block(level, item, p, 2, low).astype(jnp.bfloat16)
            stage[out, p, 0, :, high] = block(level, item, p, 1, high).astype(jnp.bfloat16)
            stage[out, p, 1, :, high] = block(level, item, p, 2, high).astype(jnp.bfloat16)
            stage[out, p, 1, :, low] = block(level, item, p, -1, low).astype(jnp.bfloat16)
        start_all(2 * level, item)

    def send_second(level, item):
        slot, out = lax.rem(item, DEPTH), lax.rem(item, SENDS)
        stage, got = ((s2, r1), (t2, q1))[level]
        wait_all(2 * level, item)
        for p in (0, 1):
            stage[out, p, 0] = (
                block(level, item, p, 1, low) + got[slot, p, 0, :, low].astype(jnp.float32)
            ).astype(jnp.bfloat16)
            stage[out, p, 1] = (
                block(level, item, p, -1, high) + got[slot, p, 1, :, high].astype(jnp.float32)
            ).astype(jnp.bfloat16)
        start_all(2 * level + 1, item)

    def finish(level, item):
        slot, out = lax.rem(item, DEPTH), lax.rem(item, SENDS)
        got1, got2 = ((r1, r2), (q1, q2))[level]
        wait_all(2 * level + 1, item)
        for p in (0, 1):
            left = (
                block(level, item, p, 0, low)
                + got2[slot, p, 0].astype(jnp.float32)
                + got1[slot, p, 1, :, low].astype(jnp.float32)
            )
            right = (
                block(level, item, p, 0, high)
                + got2[slot, p, 1].astype(jnp.float32)
                + got1[slot, p, 0, :, high].astype(jnp.float32)
            )
            if level == 0:
                part[out, p, :, low] = left
                part[out, p, :, high] = right
            else:
                fin[out, p, :, low] = left.astype(jnp.bfloat16)
                fin[out, p, :, high] = right.astype(jnp.bfloat16)

    def step(s, item):
        if s == 1:
            send_second(0, item)
        elif s == 2:
            finish(0, item)
            send_first(1, item)
        elif s == 3:
            send_second(1, item)
        elif s == 4:
            finish(1, item)
            start_all(4, item)
            for p in (0, 1):
                own_copy(p, item).start()
        else:
            wait_all(s - 1, item)
            if s == 5:
                for p in (0, 1):
                    own_copy(p, item).wait()
            if s < STEPS:
                start_all(s, item)

    deep = d_model // 2

    def x_copy(c, h):
        slot = lax.rem(c, 2)
        return pltpu.make_async_copy(
            x_hbm.at[pl.ds(pl.multiple_of(c * CHUNK, CHUNK), CHUNK), pl.ds(h * deep, deep)],
            xbuf.at[slot, :, pl.ds(h * deep, deep)],
            x_sem.at[slot, h],
        )

    def gate_copies(g, h):
        slot = lax.rem(g, 2)
        cols = pl.ds(pl.multiple_of(lax.rem(g, tiles) * TILE, TILE), TILE)
        return [
            pltpu.make_async_copy(
                w.at[pl.ds(h * deep, deep), cols],
                wgu.at[slot, pl.ds(h * deep, deep), pl.ds(n * TILE, TILE)],
                wgu_sem.at[slot, h, n],
            )
            for n, w in enumerate((wg_hbm, wu_hbm))
        ]

    def down_copies(item):
        slot = lax.rem(item, 2)
        return [
            pltpu.make_async_copy(
                wd_hbm.at[:, pl.ds(pl.multiple_of(p * half + lax.rem(item, per_chunk) * WIDTH, WIDTH), WIDTH)],
                wd.at[slot, p],
                wd_sem.at[slot, p],
            )
            for p in (0, 1)
        ]

    def start(copies):
        for one in copies:
            one.start()

    for h in (0, 1):
        x_copy(0, h).start()
        start(gate_copies(0, h))
    for h in (0, 1):
        start(gate_copies(1, h))

    def tick(t, carry):
        c, j = lax.div(t, per_chunk), lax.rem(t, per_chunk)
        item = t - per_chunk
        g = c * tiles + j
        gates = jnp.logical_and(j < tiles, c < chunks)

        def exchange(steps):
            for s in steps:
                older = item - LAG * s // 2

                @pl.when(jnp.logical_and(older >= 0, older < items))
                def _():
                    step(s, older)

        def gate_half(h):
            @pl.when(gates)
            def _():
                @pl.when(j == 0)
                def _():
                    x_copy(c, h).wait()

                for one in gate_copies(g, h):
                    one.wait()
                this = pl.ds(h * deep, deep)
                product = jnp.dot(
                    xbuf[lax.rem(c, 2), :, this], wgu[lax.rem(g, 2), this], preferred_element_type=jnp.float32
                )
                if h == 0:
                    both[...] = product
                else:
                    gate = both[:, :TILE] + product[:, :TILE]
                    up = both[:, TILE:] + product[:, TILE:]
                    hid[lax.rem(c, 2), :, pl.ds(pl.multiple_of(j * TILE, TILE), TILE)] = (
                        jax.nn.silu(gate) * up
                    ).astype(jnp.bfloat16)

                @pl.when(g + 2 < chunks * tiles)
                def _():
                    start(gate_copies(g + 2, h))

        @pl.when(jnp.logical_and(t >= per_chunk - 3, t < per_chunk - 1))
        def _():
            start(down_copies(t - (per_chunk - 3)))

        @pl.when(jnp.logical_and(j == 0, c + 1 < chunks))
        def _():
            for h in (0, 1):
                x_copy(c + 1, h).start()

        exchange(range(STEPS, 0, -2))

        @pl.when(jnp.logical_and(item >= 0, item < items))
        def _():
            for one in down_copies(item):
                one.wait()
            slot = lax.rem(item, SENDS)
            for p in (0, 1):
                term[slot, p] = jnp.dot(
                    hid[lax.rem(c + 1, 2)], wd[lax.rem(item, 2), p], preferred_element_type=jnp.float32
                )
            send_first(0, item)

            @pl.when(item + 2 < items)
            def _():
                start(down_copies(item + 2))

        gate_half(0)
        exchange(range(STEPS - 1, 0, -2))
        gate_half(1)
        return carry

    lax.fori_loop(0, per_chunk + items + LAG * STEPS // 2 + 1, tick, 0)


def solution(mesh):
    side = math.isqrt(mesh.shape["tp"])

    def block_fn(x, w_gate, w_up, w_down):
        d_model, units = w_gate.shape
        big, small, cut = CHUNK // side, CHUNK // side // side, WIDTH // 2
        bf16, f32 = jnp.bfloat16, jnp.float32
        return pl.pallas_call(
            functools.partial(kernel, side),
            out_shape=jax.ShapeDtypeStruct(x.shape, bf16),
            in_specs=[pl.BlockSpec(memory_space=pl.ANY)] * 4,
            out_specs=pl.BlockSpec(memory_space=pl.ANY),
            scratch_shapes=[
                pltpu.VMEM((2, CHUNK, d_model), bf16),
                pltpu.VMEM((2, d_model, 2 * TILE), bf16),
                pltpu.VMEM((CHUNK, 2 * TILE), f32),
                pltpu.VMEM((2, 2, units, WIDTH), bf16),
                pltpu.VMEM((2, CHUNK, units), bf16),
                pltpu.VMEM((SENDS, 2, CHUNK, WIDTH), f32),
                pltpu.VMEM((SENDS, 2, big, WIDTH), f32),
                pltpu.VMEM((SENDS, 2, 2, big, WIDTH), bf16),
                pltpu.VMEM((DEPTH, 2, 2, big, WIDTH), bf16),
                pltpu.VMEM((SENDS, 2, 2, big, cut), bf16),
                pltpu.VMEM((DEPTH, 2, 2, big, cut), bf16),
                pltpu.VMEM((SENDS, 2, 2, small, WIDTH), bf16),
                pltpu.VMEM((DEPTH, 2, 2, small, WIDTH), bf16),
                pltpu.VMEM((SENDS, 2, 2, small, cut), bf16),
                pltpu.VMEM((DEPTH, 2, 2, small, cut), bf16),
                pltpu.VMEM((SENDS, 2, small, WIDTH), bf16),
                pltpu.SemaphoreType.DMA((STEPS, 2, 2, SENDS)),
                pltpu.SemaphoreType.DMA((STEPS, 2, 2, SENDS)),
                pltpu.SemaphoreType.DMA((2, 2)),
                pltpu.SemaphoreType.DMA((2, 2, 2)),
                pltpu.SemaphoreType.DMA((2, 2)),
                pltpu.SemaphoreType.DMA((SENDS, 2)),
            ],
            compiler_params=pltpu.CompilerParams(
                collective_id=0, has_side_effects=True, vmem_limit_bytes=67_043_328
            ),
        )(x, w_gate, w_up, w_down)

    return jax.shard_map(
        block_fn,
        mesh=mesh,
        in_specs=(P("dp", None), P(None, "tp"), P(None, "tp"), P("tp", None)),
        out_specs=P("dp", None),
        check_vma=False,
    )
```

```python
import functools
import math

import jax
import jax.numpy as jnp
from jax import lax
from jax.experimental import pallas as pl
from jax.experimental.pallas import tpu as pltpu
from jax.sharding import PartitionSpec as P

CHUNK = 256
TILE = 256
WIDTH = 512
LAG = 3
DEPTH = 8
SENDS = 4
STEPS = 8
LATE = 3


def kernel(
    side, x_hbm, wg_hbm, wu_hbm, wd_hbm, y_hbm,
    xbuf, wgu, both, wd, hid, term, part, s1, r1, s2, r2, t1, q1, t2, q2, fin,
    send_sem, recv_sem, x_sem, wgu_sem, wd_sem, own_sem,
):
    rows, d_model = x_hbm.shape
    units = wg_hbm.shape[1]
    chunks = rows // CHUNK
    half = d_model // 2
    per_chunk = half // WIDTH
    tiles = units // TILE
    items = chunks * per_chunk
    early = (chunks - LATE) * per_chunk
    big, small = CHUNK // side, CHUNK // side // side
    cut = WIDTH // 2
    me = lax.axis_index("tp")
    pos = (me // side, lax.rem(me, side))

    def near(axis, step):
        at = lax.rem(pos[axis] + step + side, side)
        return at * side + pos[1] if axis == 0 else pos[0] * side + at

    def place(axis, step):
        return lax.rem(pos[axis] + step + side, side)

    barrier = pltpu.get_barrier_semaphore()
    for axis in (0, 1):
        for step in (1, -1):
            pl.semaphore_signal(
                barrier, inc=1, device_id={"tp": near(axis, step)},
                device_id_type=pl.DeviceIdType.MESH,
            )
    pl.semaphore_wait(barrier, 4)

    def copy(k, p, d, item):
        slot, out = lax.rem(item, DEPTH), lax.rem(item, SENDS)
        first, second = p, 1 - p
        axis = (first, first, second, second, second, second, first, first)[k]
        if k == 0:
            src, dst = s1.at[out, p, d], r1.at[slot, p, d]
        elif k == 1:
            src, dst = s2.at[out, p, d], r2.at[slot, p, d]
        elif k == 2:
            src, dst = t1.at[out, p, d], q1.at[slot, p, d]
        elif k == 3:
            src, dst = t2.at[out, p, d], q2.at[slot, p, d]
        else:
            row = lax.div(item, per_chunk) * CHUNK
            col = p * half + lax.rem(item, per_chunk) * WIDTH
            back = -1 if d == 0 else 1
            if k == 4:
                row += pos[first] * big + pos[second] * small
                height, wide = small, WIDTH
            elif k == 5:
                row += pos[first] * big + place(second, back) * small
                height, wide = small, cut
            elif k == 6:
                row += pos[first] * big
                height, wide = big, WIDTH
            else:
                row += place(first, back) * big
                height, wide = big, cut
            if k in (5, 7):
                col += d * cut
            dst = y_hbm.at[
                pl.ds(pl.multiple_of(row, small), height), pl.ds(pl.multiple_of(col, 128), wide)
            ]
            src = fin.at[out, p] if k == 4 else dst
        return pltpu.make_async_remote_copy(
            src_ref=src,
            dst_ref=dst,
            send_sem=send_sem.at[k, p, d, out],
            recv_sem=recv_sem.at[k, p, d, out],
            device_id={"tp": near(axis, 1 if d == 0 else -1)},
            device_id_type=pl.DeviceIdType.MESH,
        )

    def own_copy(p, item):
        out = lax.rem(item, SENDS)
        row = lax.div(item, per_chunk) * CHUNK + pos[p] * big + pos[1 - p] * small
        col = p * half + lax.rem(item, per_chunk) * WIDTH
        return pltpu.make_async_copy(
            fin.at[out, p],
            y_hbm.at[pl.ds(pl.multiple_of(row, small), small), pl.ds(pl.multiple_of(col, 128), WIDTH)],
            own_sem.at[out, p],
        )

    def start_all(k, item):
        for p in (0, 1):
            for d in (0, 1):
                copy(k, p, d, item).start()

    def wait_all(k, item):
        for p in (0, 1):
            for d in (0, 1):
                one = copy(k, p, d, item)
                one.wait_send()
                one.wait_recv()

    low, high = pl.ds(0, cut), pl.ds(cut, cut)

    def block(level, item, p, step, cols):
        slot = lax.rem(item, SENDS)
        if level == 0:
            return term[slot, p, pl.ds(pl.multiple_of(place(p, step) * big, big), big), cols]
        return part[slot, p, pl.ds(pl.multiple_of(place(1 - p, step) * small, small), small), cols]

    def send_first(level, item):
        out = lax.rem(item, SENDS)
        stage = (s1, t1)[level]
        for p in (0, 1):
            stage[out, p, 0, :, low] = block(level, item, p, 2, low).astype(jnp.bfloat16)
            stage[out, p, 0, :, high] = block(level, item, p, 1, high).astype(jnp.bfloat16)
            stage[out, p, 1, :, high] = block(level, item, p, 2, high).astype(jnp.bfloat16)
            stage[out, p, 1, :, low] = block(level, item, p, -1, low).astype(jnp.bfloat16)
        start_all(2 * level, item)

    def send_second(level, item):
        slot, out = lax.rem(item, DEPTH), lax.rem(item, SENDS)
        stage, got = ((s2, r1), (t2, q1))[level]
        wait_all(2 * level, item)
        for p in (0, 1):
            stage[out, p, 0] = (
                block(level, item, p, 1, low) + got[slot, p, 0, :, low].astype(jnp.float32)
            ).astype(jnp.bfloat16)
            stage[out, p, 1] = (
                block(level, item, p, -1, high) + got[slot, p, 1, :, high].astype(jnp.float32)
            ).astype(jnp.bfloat16)
        start_all(2 * level + 1, item)

    def finish(level, item):
        slot, out = lax.rem(item, DEPTH), lax.rem(item, SENDS)
        got1, got2 = ((r1, r2), (q1, q2))[level]
        wait_all(2 * level + 1, item)
        for p in (0, 1):
            left = (
                block(level, item, p, 0, low)
                + got2[slot, p, 0].astype(jnp.float32)
                + got1[slot, p, 1, :, low].astype(jnp.float32)
            )
            right = (
                block(level, item, p, 0, high)
                + got2[slot, p, 1].astype(jnp.float32)
                + got1[slot, p, 0, :, high].astype(jnp.float32)
            )
            if level == 0:
                part[out, p, :, low] = left
                part[out, p, :, high] = right
            else:
                fin[out, p, :, low] = left.astype(jnp.bfloat16)
                fin[out, p, :, high] = right.astype(jnp.bfloat16)

    def step(s, item):
        if s == 1:
            send_second(0, item)
        elif s == 2:
            finish(0, item)
            send_first(1, item)
        elif s == 3:
            send_second(1, item)
        elif s == 4:
            finish(1, item)
            start_all(4, item)
            for p in (0, 1):
                own_copy(p, item).start()
        else:
            wait_all(s - 1, item)
            if s == 5:
                for p in (0, 1):
                    own_copy(p, item).wait()
            if s < STEPS - 1:
                start_all(s, item)
            elif s < STEPS:

                @pl.when(item < early)
                def _():
                    start_all(s, item)

    deep = d_model // 2

    def x_copy(c, h):
        slot = lax.rem(c, 2)
        return pltpu.make_async_copy(
            x_hbm.at[pl.ds(pl.multiple_of(c * CHUNK, CHUNK), CHUNK), pl.ds(h * deep, deep)],
            xbuf.at[slot, :, pl.ds(h * deep, deep)],
            x_sem.at[slot, h],
        )

    def gate_copies(g, h):
        slot = lax.rem(g, 2)
        cols = pl.ds(pl.multiple_of(lax.rem(g, tiles) * TILE, TILE), TILE)
        return [
            pltpu.make_async_copy(
                w.at[pl.ds(h * deep, deep), cols],
                wgu.at[slot, pl.ds(h * deep, deep), pl.ds(n * TILE, TILE)],
                wgu_sem.at[slot, h, n],
            )
            for n, w in enumerate((wg_hbm, wu_hbm))
        ]

    def down_copies(item):
        slot = lax.rem(item, 2)
        return [
            pltpu.make_async_copy(
                wd_hbm.at[:, pl.ds(pl.multiple_of(p * half + lax.rem(item, per_chunk) * WIDTH, WIDTH), WIDTH)],
                wd.at[slot, p],
                wd_sem.at[slot, p],
            )
            for p in (0, 1)
        ]

    def start(copies):
        for one in copies:
            one.start()

    for h in (0, 1):
        x_copy(0, h).start()
        start(gate_copies(0, h))
    for h in (0, 1):
        start(gate_copies(1, h))

    def tick(t, carry):
        c, j = lax.div(t, per_chunk), lax.rem(t, per_chunk)
        item = t - per_chunk
        g = c * tiles + j
        gates = jnp.logical_and(j < tiles, c < chunks)

        def exchange(steps):
            for s in steps:
                older = item - LAG * s // 2

                @pl.when(jnp.logical_and(older >= 0, older < (items if s < STEPS else early)))
                def _():
                    step(s, older)

        def gate_half(h):
            @pl.when(gates)
            def _():
                @pl.when(j == 0)
                def _():
                    x_copy(c, h).wait()

                for one in gate_copies(g, h):
                    one.wait()
                this = pl.ds(h * deep, deep)
                product = jnp.dot(
                    xbuf[lax.rem(c, 2), :, this], wgu[lax.rem(g, 2), this], preferred_element_type=jnp.float32
                )
                if h == 0:
                    both[...] = product
                else:
                    gate = both[:, :TILE] + product[:, :TILE]
                    up = both[:, TILE:] + product[:, TILE:]
                    hid[lax.rem(c, 2), :, pl.ds(pl.multiple_of(j * TILE, TILE), TILE)] = (
                        jax.nn.silu(gate) * up
                    ).astype(jnp.bfloat16)

                @pl.when(g + 2 < chunks * tiles)
                def _():
                    start(gate_copies(g + 2, h))

        @pl.when(jnp.logical_and(t >= per_chunk - 3, t < per_chunk - 1))
        def _():
            start(down_copies(t - (per_chunk - 3)))

        @pl.when(jnp.logical_and(j == 0, c + 1 < chunks))
        def _():
            for h in (0, 1):
                x_copy(c + 1, h).start()

        exchange(range(STEPS, 0, -2))

        @pl.when(jnp.logical_and(item >= 0, item < items))
        def _():
            for one in down_copies(item):
                one.wait()
            slot = lax.rem(item, SENDS)
            for p in (0, 1):
                term[slot, p] = jnp.dot(
                    hid[lax.rem(c + 1, 2)], wd[lax.rem(item, 2), p], preferred_element_type=jnp.float32
                )
            send_first(0, item)

            @pl.when(item + 2 < items)
            def _():
                start(down_copies(item + 2))

        gate_half(0)
        exchange(range(STEPS - 1, 0, -2))
        gate_half(1)
        return carry

    lax.fori_loop(0, per_chunk + items + LAG * (STEPS - 1) // 2 + 1, tick, 0)


def copy_kernel(from_hbm, to_hbm, held, in_sem, out_sem):
    slots, high, _ = held.shape
    ahead = slots // 2
    blocks = from_hbm.shape[0] // high

    def rows(i):
        return pl.ds(pl.multiple_of(i * high, high), high)

    def read(i):
        slot = lax.rem(i, slots)
        return pltpu.make_async_copy(from_hbm.at[rows(i)], held.at[slot], in_sem.at[slot])

    def write(i):
        slot = lax.rem(i, slots)
        return pltpu.make_async_copy(held.at[slot], to_hbm.at[rows(i)], out_sem.at[slot])

    for i in range(ahead):
        read(i).start()

    def move(i, carry):
        @pl.when(i >= ahead)
        def _():
            write(i - ahead).wait()

        @pl.when(i + ahead < blocks)
        def _():
            read(i + ahead).start()

        @pl.when(i < blocks)
        def _():
            read(i).wait()
            write(i).start()

        return carry

    lax.fori_loop(0, blocks + ahead, move, 0)


def copied(y):
    rows, d_model = y.shape
    high, slots = CHUNK // 8, 32
    return pl.pallas_call(
        copy_kernel,
        out_shape=jax.ShapeDtypeStruct(y.shape, y.dtype),
        in_specs=[pl.BlockSpec(memory_space=pl.ANY)],
        out_specs=pl.BlockSpec(memory_space=pl.ANY),
        scratch_shapes=[
            pltpu.VMEM((slots, high, d_model), y.dtype),
            pltpu.SemaphoreType.DMA((slots,)),
            pltpu.SemaphoreType.DMA((slots,)),
        ],
        cost_estimate=pl.CostEstimate(
            flops=600 * y.size, bytes_accessed=4 * y.size, transcendentals=0
        ),
    )(y)


def last_step(side, y):
    rows, d_model = y.shape
    chunks, big, half = rows // CHUNK, CHUNK // side, d_model // 2
    cut = half // 2
    me = lax.axis_index("tp")
    pos = (me // side, lax.rem(me, side))
    view = y.reshape(chunks, CHUNK, d_model)
    moved = []
    for p in (0, 1):
        for d, step in enumerate((1, -1)):
            row = lax.rem(pos[p] - step + side, side) * big
            piece = lax.dynamic_slice(
                view, (chunks - LATE, row, p * half + d * cut), (LATE, big, cut)
            )
            pairs = []
            for x in range(side):
                for v in range(side):
                    to = ((x + step) % side, v) if p == 0 else (x, (v + step) % side)
                    pairs.append((x * side + v, to[0] * side + to[1]))
            moved.append((p, d, lax.ppermute(piece, "tp", pairs)))
    z = copied(y).reshape(chunks, CHUNK, d_model)
    for p, d, piece in moved:
        row = lax.rem(pos[p] + 2, side) * big
        z = lax.dynamic_update_slice(z, piece, (chunks - LATE, row, p * half + d * cut))
    return z.reshape(rows, d_model)


def solution(mesh):
    side = math.isqrt(mesh.shape["tp"])

    def block_fn(x, w_gate, w_up, w_down):
        d_model, units = w_gate.shape
        big, small, cut = CHUNK // side, CHUNK // side // side, WIDTH // 2
        bf16, f32 = jnp.bfloat16, jnp.float32
        y = pl.pallas_call(
            functools.partial(kernel, side),
            out_shape=jax.ShapeDtypeStruct(x.shape, bf16),
            in_specs=[pl.BlockSpec(memory_space=pl.ANY)] * 4,
            out_specs=pl.BlockSpec(memory_space=pl.ANY),
            scratch_shapes=[
                pltpu.VMEM((2, CHUNK, d_model), bf16),
                pltpu.VMEM((2, d_model, 2 * TILE), bf16),
                pltpu.VMEM((CHUNK, 2 * TILE), f32),
                pltpu.VMEM((2, 2, units, WIDTH), bf16),
                pltpu.VMEM((2, CHUNK, units), bf16),
                pltpu.VMEM((SENDS, 2, CHUNK, WIDTH), f32),
                pltpu.VMEM((SENDS, 2, big, WIDTH), f32),
                pltpu.VMEM((SENDS, 2, 2, big, WIDTH), bf16),
                pltpu.VMEM((DEPTH, 2, 2, big, WIDTH), bf16),
                pltpu.VMEM((SENDS, 2, 2, big, cut), bf16),
                pltpu.VMEM((DEPTH, 2, 2, big, cut), bf16),
                pltpu.VMEM((SENDS, 2, 2, small, WIDTH), bf16),
                pltpu.VMEM((DEPTH, 2, 2, small, WIDTH), bf16),
                pltpu.VMEM((SENDS, 2, 2, small, cut), bf16),
                pltpu.VMEM((DEPTH, 2, 2, small, cut), bf16),
                pltpu.VMEM((SENDS, 2, small, WIDTH), bf16),
                pltpu.SemaphoreType.DMA((STEPS, 2, 2, SENDS)),
                pltpu.SemaphoreType.DMA((STEPS, 2, 2, SENDS)),
                pltpu.SemaphoreType.DMA((2, 2)),
                pltpu.SemaphoreType.DMA((2, 2, 2)),
                pltpu.SemaphoreType.DMA((2, 2)),
                pltpu.SemaphoreType.DMA((SENDS, 2)),
            ],
            compiler_params=pltpu.CompilerParams(
                collective_id=0, has_side_effects=True, vmem_limit_bytes=67_043_328
            ),
        )(x, w_gate, w_up, w_down)
        return last_step(side, y)

    return jax.shard_map(
        block_fn,
        mesh=mesh,
        in_specs=(P("dp", None), P(None, "tp"), P(None, "tp"), P("tp", None)),
        out_specs=P("dp", None),
        check_vma=False,
    )
```
